256 devices in a mesh: range: 128 (over z, y, x), chip: 2 (over core).
Axes of the slice: x: 4, y: 4, z: 8, core: 2. Of those that a mesh axis runs over, the one named last changes fastest.
Arguments:
- mode_tables: bfloat16 [256, 2048, 768], P('range', None, 'chip'), may hold values from -1 to 1
- attenuation: float32 [256, 768], P('range'), may hold values from 0 to 1, as said below
- excitation: float32 [768, 128], replicated, may hold values from -6 to 6
Outputs:
- fields: float32 [256, 2048, 128], P('range', 'chip')
The draws below stay inside these ranges and needn't reach their ends.
Inputs may be any that keep to these rules, and one draw needn't show every extreme that they name: attenuation rates, positive.
All inputs are finite; a program needn't handle non-finite values.
Results may differ from the reference program's by a relative error of at most 0.0029.
Values may be sent and summed in bfloat16 or wider, within the bound.
No kernel may reach another device: no remote copies, remote signals or barrier semaphores. Data moves between devices by JAX's collectives and lax.ppermute only.
A program may use at most 64 MiB of HBM per device.

```python
import math
import jax
import jax.numpy as jnp
from jax import lax

MODES = 768
HEIGHTS = 2048
SOURCES = 128
RANGE_SEGMENTS = 256


def draw_mode_tables(key, part):
    base_key, noise_key = jax.random.split(jax.random.fold_in(key, 11))
    starting_value = jax.random.normal(base_key, (HEIGHTS, MODES), jnp.float32)
    ortho, _ = jnp.linalg.qr(starting_value)
    noise = jax.random.normal(noise_key, (RANGE_SEGMENTS, HEIGHTS, MODES), jnp.float32) * (0.082 / math.sqrt(HEIGHTS))
    return (ortho[None] + noise).astype(jnp.bfloat16)


def draw_attenuation(key, part):
    first_key, second_key, tertiary_key = jax.random.split(jax.random.fold_in(key, 23), 3)
    lowest = 0.3 / RANGE_SEGMENTS
    highest_rate = 0.03
    starting_value = jnp.exp(jax.random.uniform(first_key, (MODES,), jnp.float32, math.log(lowest), math.log(max(highest_rate, 2.0 * lowest))))
    multiplier = jnp.exp(jax.random.uniform(second_key, (RANGE_SEGMENTS, MODES), jnp.float32, math.log(0.5), math.log(2.0)))
    spike_positions = jax.random.randint(tertiary_key, (3,), 0, RANGE_SEGMENTS)
    spike_count = jnp.sum((jnp.arange(RANGE_SEGMENTS)[:, None] == spike_positions[None, :]).astype(jnp.float32), axis=1)
    return starting_value[None, :] * multiplier + 0.3 * spike_count[:, None]


def gaussian(key, extent, width, reach, held_as=jnp.bfloat16):
    return jnp.clip(width * jax.random.normal(key, extent, jnp.float32), -reach, reach).astype(held_as)


def setup_inputs(seed: int = 0) -> dict:
    splits = jax.random.split(jax.random.key(seed), 4)
    mode_tables = draw_mode_tables(jax.random.fold_in(splits[3], 71), 0)
    attenuation = draw_attenuation(jax.random.fold_in(splits[3], 71), 0)
    excitation = gaussian(splits[2], (MODES, SOURCES), 1.0, 6.0, jnp.float32)
    return dict(mode_tables=mode_tables, attenuation=attenuation, excitation=excitation)


highest = lax.Precision.HIGHEST

def widen(table):
    return table.astype(jnp.float32)

def field_of(table, amplitude):
    rounded = lax.optimization_barrier(amplitude.astype(jnp.bfloat16))
    return jnp.dot(widen(table), rounded.astype(jnp.float32), precision=highest)

def reference(mode_tables, attenuation, excitation):
    first_amplitude = jnp.exp(-attenuation[0])[:, None] * excitation

    def advance(state, inputs):
        amplitude, earlier = state
        current, damping_rates = inputs
        intersection = jnp.dot(widen(current).T, widen(earlier), precision=highest)
        matrix = jnp.exp(-damping_rates)[:, None] * intersection
        amplitude = jnp.dot(matrix, amplitude, precision=highest)
        return ((amplitude, current), field_of(current, amplitude))
    initial = (first_amplitude, mode_tables[0])
    _, later_fields = lax.scan(advance, initial, (mode_tables[1:], attenuation[1:]))
    first_field = field_of(mode_tables[0], first_amplitude)
    return jnp.concatenate([first_field[None], later_fields], axis=0)
```

```python
import functools

import jax
import jax.numpy as jnp
from jax import lax
from jax.experimental import pallas as pl
from jax.experimental.pallas import tpu as pltpu
from jax.sharding import PartitionSpec as P

INTERPRET = False
f32, bf16 = jnp.float32, jnp.bfloat16


def from_behind(value, steps):
    count = lax.axis_size("range")
    return lax.ppermute(value, "range", [(i, i + steps) for i in range(count - steps)])


def from_partner(value):
    return lax.ppermute(value, "chip", [(0, 1), (1, 0)])


def split(x):
    hi = x.astype(bf16)
    return hi, (x - hi.astype(f32)).astype(bf16)


def mm(a, b):
    return jnp.dot(a, b, preferred_element_type=f32)


def mm3(lhi, llo, rhi, rlo):
    rows = lhi.shape[0]
    both = mm(jnp.concatenate([lhi, llo], axis=0), rhi)
    return both[:rows] + (both[rows:] + mm(lhi, rlo))


def swap_cols(x):
    half = x.shape[1] // 2
    return jnp.concatenate([x[:, half:], x[:, :half]], axis=1)


def call(kernel, out, *args):
    spec = {4: pltpu.SMEM}
    in_specs = [
        pl.BlockSpec(memory_space=pltpu.SMEM if a.dtype == jnp.int32 else pltpu.VMEM) for a in args
    ]
    many = isinstance(out, (tuple, list))
    out_specs = [pl.BlockSpec(memory_space=pltpu.VMEM) for _ in out] if many else pl.BlockSpec(memory_space=pltpu.VMEM)
    return pl.pallas_call(
        kernel, out_shape=out, in_specs=in_specs, out_specs=out_specs, interpret=INTERPRET
    )(*args)


def couple_kernel(own_ref, other_ref, out_ref):
    half = own_ref.shape[1]
    for cols, x in ((slice(0, half), own_ref[...]),):
        hi, lo = split(x)
        out_ref[0, :, cols] = hi
        out_ref[1, :, cols] = lo
    for into, out_of in ((slice(0, half), slice(half, 2 * half)), (slice(half, 2 * half), slice(0, half))):
        hi, lo = split(other_ref[out_of, :])
        out_ref[0, into, half:] = hi
        out_ref[1, into, half:] = lo


def row_couple_kernel(own_ref, other_ref, out_ref):
    half = own_ref.shape[0]
    hi, lo = split(own_ref[...])
    out_ref[0, :half] = hi
    out_ref[1, :half] = lo
    hi, lo = split(swap_cols(other_ref[...]))
    out_ref[0, half:] = hi
    out_ref[1, half:] = lo


def local_kernel(kt_ref, g_ref, out_ref):
    khi, klo = split(kt_ref[...])
    hi, lo = split(mm3(khi, klo, g_ref[0], g_ref[1]))
    out_ref[0] = hi
    out_ref[1] = lo


def round_kernel(which, flags_ref, own_ref, other_ref, right_ref, out_ref):
    @pl.when(flags_ref[which] == 0)
    def _():
        out_ref[...] = own_ref[...]

    @pl.when(flags_ref[which] != 0)
    def _():
        whi = jnp.concatenate([own_ref[0], swap_cols(other_ref[0])], axis=0)
        wlo = jnp.concatenate([own_ref[1], swap_cols(other_ref[1])], axis=0)
        hi, lo = split(mm3(right_ref[0], right_ref[1], whi, wlo))
        out_ref[0] = hi
        out_ref[1] = lo


def launch_kernel(own_ref, other_ref, state_ref, reached_ref, window_ref):
    half = own_ref.shape[1]
    for i in range(2):
        window_ref[i, :half] = own_ref[i]
        window_ref[i, half:] = swap_cols(other_ref[i])
    shi, slo = split(state_ref[...])
    reached_ref[...] = mm3(shi, slo, window_ref[0], window_ref[1])


def hop_kernel(which, flags_ref, incoming_ref, reached_ref, window_ref, out_ref):
    @pl.when(flags_ref[which] == 0)
    def _():
        out_ref[...] = reached_ref[...]

    @pl.when(flags_ref[which] != 0)
    def _():
        shi, slo = split(incoming_ref[...])
        out_ref[...] = mm3(shi, slo, window_ref[0], window_ref[1])


def last_kernel(which, flags_ref, start_ref, arriving_ref, reached_ref, damping_ref, k_ref, out_ref):
    first = flags_ref[which] != 0
    v = jnp.where(first, start_ref[...], arriving_ref[...])
    shi, slo = split(v)
    out_ref[0] = (mm3(shi, slo, k_ref[0], k_ref[1]) * damping_ref[...]).astype(bf16)
    out_ref[1] = reached_ref[...].astype(bf16)


def on_device(mode_tables, attenuation, excitation):
    _, heights, half = mode_tables.shape
    modes = 2 * half
    count = lax.axis_size("range")
    position = lax.axis_index("range")
    core = lax.axis_index("chip")
    rounds = (count - 1).bit_length()
    window_rounds = max(min(rounds, 4), rounds - 3)
    stride = 2**window_rounds
    hops = range(1, -(-count // stride))
    flags = jnp.stack(
        [(position >= 2**i) for i in range(window_rounds)]
        + [position // stride == h for h in hops]
        + [position == 0]
    ).astype(jnp.int32)

    table_a, table_b = mode_tables[0], mode_tables[1]
    earlier = from_behind(table_b, 1)
    other_a = from_partner(table_a)
    rows = heights // 2
    theirs = lax.dynamic_slice_in_dim(table_b, (1 - core) * rows, rows, 0)
    other_rows_b = from_partner(theirs)

    damping = jnp.exp(-attenuation)
    damping = jnp.where(core == 0, damping, jnp.roll(damping, half, axis=1))
    sources = excitation.shape[1] // 2
    start = lax.dynamic_slice_in_dim(excitation, core * sources, sources, 1).T
    start = jnp.where(core == 0, start, jnp.roll(start, half, axis=1))

    def overlap(a, b):
        return jnp.einsum("hi,hj->ij", a, b, preferred_element_type=f32)

    damping_a, damping_b = damping[0], damping[1, :half]
    inner = jnp.concatenate([overlap(table_a, table_b), overlap(other_a, table_b)], axis=0)
    inner = inner * damping_a[:, None] * damping_b[None, :]
    inner_other = from_partner(inner)
    matrix = jax.ShapeDtypeStruct((2, modes, modes), bf16)
    panel = jax.ShapeDtypeStruct((2, half, modes), bf16)
    inner = call(couple_kernel, matrix, inner, inner_other)

    k = jnp.concatenate([overlap(earlier, table_a), overlap(earlier, other_a)], axis=1)
    k = jnp.where(position == 0, jnp.eye(half, modes, dtype=f32), k)
    k_other = from_partner(k)
    window = call(local_kernel, panel, k, inner)
    for i in range(window_rounds):
        behind = from_behind(window, 2**i)
        other = from_partner(window)
        window = call(functools.partial(round_kernel, i), panel, flags, window, other, behind)
        if i == 0:
            k = call(row_couple_kernel, matrix, k, k_other)
    other = from_partner(window)
    state = jax.ShapeDtypeStruct((sources, modes), f32)
    reached, window = call(launch_kernel, (state, matrix), window, other, start)
    for n, _ in enumerate(hops):
        incoming = from_behind(reached, stride)
        reached = call(functools.partial(hop_kernel, window_rounds + n), state, flags, incoming, reached, window)
    arriving = from_behind(reached, 1)
    amplitude = call(
        functools.partial(last_kernel, flags.shape[0] - 1),
        jax.ShapeDtypeStruct((2, sources, modes), bf16),
        flags, start, arriving, reached, damping[:1], k,
    )
    others = from_partner(amplitude)
    others = jnp.concatenate([others[:, :, half:], others[:, :, :half]], axis=2)
    low, high = jnp.where(core == 0, amplitude, others), jnp.where(core == 0, others, amplitude)
    amplitude = jnp.concatenate([low, high], axis=1)

    own_rows = lax.dynamic_slice_in_dim(mode_tables, core * rows, rows, 1)
    other_rows_a = lax.dynamic_slice_in_dim(other_a, core * rows, rows, 0)
    whole_rows = jnp.concatenate([own_rows, jnp.stack([other_rows_a, other_rows_b])], axis=2)
    return jnp.einsum("shm,scm->shc", whole_rows, amplitude, preferred_element_type=f32)


def solution(mesh):
    placed = (P("range", None, "chip"), P("range", None), P())
    return jax.shard_map(
        on_device, mesh=mesh, in_specs=placed, out_specs=P("range", "chip", None), check_vma=False
    )
```

```python
import functools

import jax
import jax.numpy as jnp
from jax import lax
from jax.experimental import pallas as pl
from jax.experimental.pallas import tpu as pltpu
from jax.sharding import PartitionSpec as P

INTERPRET = False
f32, bf16 = jnp.float32, jnp.bfloat16


def from_behind(value, steps):
    count = lax.axis_size("range")
    return lax.ppermute(value, "range", [(i, (i + steps) % count) for i in range(count)])


def from_partner(value):
    return lax.ppermute(value, "chip", [(0, 1), (1, 0)])


def split(x):
    hi = x.astype(bf16)
    return hi, (x - hi.astype(f32)).astype(bf16)


def mm(a, b):
    return jnp.dot(a, b, preferred_element_type=f32)


def mm3(lhi, llo, rhi, rlo):
    rows = lhi.shape[0]
    both = mm(jnp.concatenate([lhi, llo], axis=0), rhi)
    return both[:rows] + (both[rows:] + mm(lhi, rlo))


def swap_cols(x):
    half = x.shape[1] // 2
    return jnp.concatenate([x[:, half:], x[:, :half]], axis=1)


def call(kernel, out, *args):
    in_specs = [
        pl.BlockSpec(memory_space=pltpu.SMEM if a.dtype == jnp.int32 else pltpu.VMEM) for a in args
    ]
    out_specs = [pl.BlockSpec(memory_space=pltpu.VMEM) for _ in out]
    shapes = list(out)
    if not INTERPRET:
        shapes = [pltpu.VMEM(o.shape, o.dtype) for o in out]
        args = [
            a if a.dtype == jnp.int32 else pltpu.with_memory_space_constraint(a, pltpu.VMEM) for a in args
        ]
    outs = pl.pallas_call(
        kernel, out_shape=shapes, in_specs=in_specs, out_specs=out_specs, interpret=INTERPRET,
        compiler_params=pltpu.CompilerParams(vmem_limit_bytes=24 * 2**20)
    )(*args)
    return outs if len(out) > 1 else outs[0]


def load_kernel(tables_ref, a_ref, first_ref, second_ref, sems):
    cut = first_ref.shape[1]
    copies = [
        pltpu.make_async_copy(tables_ref.at[1, :, :cut], first_ref, sems.at[0]),
        pltpu.make_async_copy(tables_ref.at[1, :, cut:], second_ref, sems.at[1]),
        pltpu.make_async_copy(tables_ref.at[0], a_ref, sems.at[2]),
    ]
    for c in copies:
        c.start()
    for c in copies:
        c.wait()


def load_tables(tables, cut):
    if INTERPRET:
        return tables[0], tables[1][:, :cut], tables[1][:, cut:]
    _, heights, half = tables.shape
    vmem = pl.BlockSpec(memory_space=pltpu.VMEM)
    return pl.pallas_call(
        load_kernel,
        out_shape=[pltpu.VMEM((heights, n), tables.dtype) for n in (half, cut, half - cut)],
        in_specs=[pl.BlockSpec(memory_space=pl.ANY)],
        out_specs=[vmem] * 3,
        scratch_shapes=[pltpu.SemaphoreType.DMA((3,))],
        compiler_params=pltpu.CompilerParams(vmem_limit_bytes=24 * 2**20),
    )(tables)


def couple_kernel(own_ref, other_ref, out_ref):
    half = own_ref.shape[1]
    for cols, x in ((slice(0, half), own_ref[...]),):
        hi, lo = split(x)
        out_ref[0, :, cols] = hi
        out_ref[1, :, cols] = lo
    for into, out_of in ((slice(0, half), slice(half, 2 * half)), (slice(half, 2 * half), slice(0, half))):
        hi, lo = split(other_ref[out_of, :])
        out_ref[0, into, half:] = hi
        out_ref[1, into, half:] = lo


def row_couple_kernel(own_ref, other_ref, out_ref):
    half = own_ref.shape[0]
    hi, lo = split(own_ref[...])
    out_ref[0, :half] = hi
    out_ref[1, :half] = lo
    hi, lo = split(swap_cols(other_ref[...]))
    out_ref[0, half:] = hi
    out_ref[1, half:] = lo


PAD = 16


def on_diagonal(shape, first):
    return lax.broadcasted_iota(jnp.int32, shape, 0) + first == lax.broadcasted_iota(jnp.int32, shape, 1)


def pack(z, first, ref):
    rows = z.shape[0]
    top = jnp.maximum(jnp.max(jnp.abs(z), axis=(0, 1), keepdims=True), 1e-30)
    exponent = jnp.floor(jnp.log2(top)) - 14.0
    z = z * jnp.exp2(-exponent)
    mask = on_diagonal(z.shape, first)
    diagonal = jnp.sum(jnp.where(mask, z, 0.0), axis=0, keepdims=True)
    hi = diagonal.astype(bf16).astype(f32)
    shape = (PAD, z.shape[1])
    row = lax.broadcasted_iota(jnp.int32, shape, 0)
    ref[:rows] = jnp.where(mask, 0.0, z)
    ref[rows:] = jnp.where(row == 0, exponent, jnp.where(row == 1, hi, jnp.where(row == 2, diagonal - hi, 0.0)))


def unpack(ref, first):
    rows = ref.shape[0] - PAD
    z = ref[:rows]
    diagonal = ref[rows + 1 : rows + 2] + ref[rows + 2 : rows + 3]
    return jnp.where(on_diagonal(z.shape, first), diagonal, z), jnp.exp2(ref[rows : rows + 1, :1])


def ahead_of(packed, steps):
    return from_behind(packed.astype(jnp.float16), steps).astype(f32)


def local_kernel(first, kt_ref, g_ref, out_ref, packed_ref):
    khi, klo = split(kt_ref[...])
    z = mm3(khi, klo, g_ref[0], g_ref[1])
    out_ref[0], out_ref[1] = split(z)
    pack(z, first, packed_ref)


def assembled(own_a, own_b, other_a, other_b, part):
    return jnp.concatenate(
        [own_a[part], own_b[part], swap_cols(other_a[part]), swap_cols(other_b[part])], axis=0
    )


def round_kernel(which, chunk, first, flags_ref, oa_ref, ob_ref, xa_ref, xb_ref, right_ref, *rest):
    own_ref = (oa_ref, ob_ref)[chunk]
    out_ref = rest[-1] if len(rest) == 1 else rest[1]

    @pl.when(flags_ref[which] == 0)
    def _():
        out_ref[...] = own_ref[...]
        if len(rest) > 1:
            rest[2][...] = rest[0][...]

    @pl.when(flags_ref[which] != 0)
    def _():
        right, scale = unpack(right_ref, first)
        rhi, rlo = split(right)
        whi, wlo = (assembled(oa_ref, ob_ref, xa_ref, xb_ref, part) for part in range(2))
        z = mm3(rhi, rlo, whi, wlo) * scale
        out_ref[0], out_ref[1] = split(z)
        if len(rest) > 1:
            pack(z, first, rest[2])


def launch_kernel(oa_ref, ob_ref, xa_ref, xb_ref, state_ref, reached_ref, window_ref):
    for part in range(2):
        window_ref[part] = assembled(oa_ref, ob_ref, xa_ref, xb_ref, part)
    shi, slo = split(state_ref[...])
    reached_ref[...] = mm3(shi, slo, window_ref[0], window_ref[1])


def hop_kernel(which, flags_ref, incoming_ref, reached_ref, window_ref, out_ref):
    @pl.when(flags_ref[which] == 0)
    def _():
        out_ref[...] = reached_ref[...]

    @pl.when(flags_ref[which] != 0)
    def _():
        shi, slo = split(incoming_ref[...])
        out_ref[...] = mm3(shi, slo, window_ref[0], window_ref[1])


def last_kernel(which, flags_ref, start_ref, arriving_ref, reached_ref, damping_ref, k_ref, out_ref):
    first = flags_ref[which] != 0
    v = jnp.where(first, start_ref[...], arriving_ref[...])
    shi, slo = split(v)
    out_ref[0] = (mm3(shi, slo, k_ref[0], k_ref[1]) * damping_ref[...]).astype(bf16)
    out_ref[1] = reached_ref[...].astype(bf16)


def on_device(mode_tables, attenuation, excitation):
    _, heights, half = mode_tables.shape
    modes = 2 * half
    count = lax.axis_size("range")
    position = lax.axis_index("range")
    core = lax.axis_index("chip")
    rounds = (count - 1).bit_length()
    window_rounds = max(min(rounds, 4), rounds - 3)
    stride = 2**window_rounds
    hops = range(1, -(-count // stride))
    flags = jnp.stack(
        [(position >= 2**i) for i in range(window_rounds)]
        + [position // stride == h for h in hops]
        + [position == 0]
    ).astype(jnp.int32)

    cuts = (0, half * 2 // 3, half)
    table_a, *table_b = load_tables(mode_tables, cuts[1])
    earlier = [from_behind(t, 1) for t in table_b]
    table_b = jnp.concatenate(table_b, axis=1)
    other_a = from_partner(table_a)
    rows = heights // 2
    theirs = lax.dynamic_slice_in_dim(table_b, (1 - core) * rows, rows, 0)
    other_rows_b = from_partner(theirs)

    damping = jnp.exp(-attenuation)
    damping = jnp.where(core == 0, damping, jnp.roll(damping, half, axis=1))
    sources = excitation.shape[1] // 2
    start = lax.dynamic_slice_in_dim(excitation, core * sources, sources, 1).T
    start = jnp.where(core == 0, start, jnp.roll(start, half, axis=1))

    def overlap(a, b):
        return jnp.einsum("hi,hj->ij", a, b, preferred_element_type=f32)

    damping_a, damping_b = damping[0], damping[1, :half]
    inner = jnp.concatenate([overlap(table_a, table_b), overlap(other_a, table_b)], axis=0)
    inner = inner * damping_a[:, None] * damping_b[None, :]
    inner_other = from_partner(inner)
    matrix = jax.ShapeDtypeStruct((2, modes, modes), bf16)
    inner = call(couple_kernel, (matrix,), inner, inner_other)

    both_a = jnp.concatenate([table_a, other_a], axis=1)
    own_rows = lax.dynamic_slice_in_dim(jnp.stack([table_a, table_b]), core * rows, rows, 1)
    other_rows_a = lax.dynamic_slice_in_dim(other_a, core * rows, rows, 0)
    whole_rows = jnp.concatenate([own_rows, jnp.stack([other_rows_a, other_rows_b])], axis=2)
    earlier[0], both_a, whole_rows, start, inner = lax.optimization_barrier(
        (earlier[0], both_a, whole_rows, start, inner)
    )

    chunks = range(2)
    sizes = [cuts[c + 1] - cuts[c] for c in chunks]
    panels = [jax.ShapeDtypeStruct((2, n, modes), bf16) for n in sizes]
    packs = [jax.ShapeDtypeStruct((n + PAD, modes), f32) for n in sizes]
    k, window, packed = [None] * 2, [None] * 2, [None] * 2
    for c in chunks:
        k[c] = overlap(earlier[c], both_a)
        k[c] = jnp.where(position == 0, jnp.eye(sizes[c], modes, cuts[c], dtype=f32), k[c])
        window[c], packed[c] = call(
            functools.partial(local_kernel, cuts[c]), (panels[c], packs[c]), k[c], inner
        )
    k = jnp.concatenate(k, axis=0)
    k_other = from_partner(k)
    for i in range(window_rounds):
        behind = [ahead_of(packed[c], 2**i) for c in chunks]
        other = [from_partner(window[c]) for c in chunks]
        if i == 0:
            behind[1], k_other = lax.optimization_barrier((behind[1], k_other))
        if i == 1:
            behind[0], k = lax.optimization_barrier((behind[0], call(row_couple_kernel, (matrix,), k, k_other)))
        last = i == window_rounds - 1
        outs = [
            call(
                functools.partial(round_kernel, i, c, cuts[c]),
                (panels[c],) if last else (panels[c], packs[c]),
                flags, *window, *other, behind[c], *(() if last else (packed[c],)),
            )
            for c in chunks
        ]
        window, packed = (outs, None) if last else zip(*outs)
    other = [from_partner(window[c]) for c in chunks]
    state = jax.ShapeDtypeStruct((sources, modes), f32)
    reached, window = call(launch_kernel, (state, matrix), *window, *other, start)
    for n, _ in enumerate(hops):
        incoming = from_behind(reached, stride)
        reached = call(functools.partial(hop_kernel, window_rounds + n), (state,), flags, incoming, reached, window)
    arriving = from_behind(reached, 1)
    amplitude = call(
        functools.partial(last_kernel, flags.shape[0] - 1),
        (jax.ShapeDtypeStruct((2, sources, modes), bf16),),
        flags, start, arriving, reached, damping[:1], k,
    )
    others = from_partner(amplitude)
    others = jnp.concatenate([others[:, :, half:], others[:, :, :half]], axis=2)
    low, high = jnp.where(core == 0, amplitude, others), jnp.where(core == 0, others, amplitude)
    amplitude = jnp.concatenate([low, high], axis=1)

    return jnp.einsum("shm,scm->shc", whole_rows, amplitude, preferred_element_type=f32)


def solution(mesh):
    placed = (P("range", None, "chip"), P("range", None), P())
    return jax.shard_map(
        on_device, mesh=mesh, in_specs=placed, out_specs=P("range", "chip", None), check_vma=False
    )
```

```python
import functools

import jax
import jax.numpy as jnp
from jax import lax
from jax.experimental import pallas as pl
from jax.experimental.pallas import tpu as pltpu
from jax.sharding import PartitionSpec as P

INTERPRET = False
f32, bf16 = jnp.float32, jnp.bfloat16


SIDE = 4
PLANE = SIDE * SIDE


def from_behind(value, steps):
    count = lax.axis_size("range")
    return lax.ppermute(value, "range", [(i, (i + steps) % count) for i in range(count)])


def around(value, unit, steps):
    count = lax.axis_size("range")

    def target(i):
        place = i // unit % SIDE
        return i + unit * ((place + steps) % SIDE - place)

    return lax.ppermute(value, "range", [(i, target(i)) for i in range(count)])


def from_partner(value):
    return lax.ppermute(value, "chip", [(0, 1), (1, 0)])


def split(x):
    hi = x.astype(bf16)
    return hi, (x - hi.astype(f32)).astype(bf16)


def mm(a, b):
    return jnp.dot(a, b, preferred_element_type=f32)


def mm3(lhi, llo, rhi, rlo):
    rows = lhi.shape[0]
    both = mm(jnp.concatenate([lhi, llo], axis=0), rhi)
    return both[:rows] + (both[rows:] + mm(lhi, rlo))


def swap_cols(x):
    half = x.shape[1] // 2
    return jnp.concatenate([x[:, half:], x[:, :half]], axis=1)


def call(kernel, out, *args, scratch=(), limit=12, aliases=None):
    in_specs = [
        pl.BlockSpec(memory_space=pltpu.SMEM if a.dtype == jnp.int32 else pltpu.VMEM) for a in args
    ]
    out_specs = [pl.BlockSpec(memory_space=pltpu.VMEM) for _ in out]
    shapes = list(out)
    if not INTERPRET:
        shapes = [pltpu.VMEM(o.shape, o.dtype) for o in out]
        args = [
            a if a.dtype == jnp.int32 else pltpu.with_memory_space_constraint(a, pltpu.VMEM) for a in args
        ]
    outs = pl.pallas_call(
        kernel, out_shape=shapes, in_specs=in_specs, out_specs=out_specs, interpret=INTERPRET,
        compiler_params=pltpu.CompilerParams(vmem_limit_bytes=limit * 2**20),
        scratch_shapes=scratch,
        input_output_aliases=aliases or {},
    )(*args)
    return outs if len(out) > 1 else outs[0]


def load_kernel(tables_ref, a_ref, first_ref, second_ref, sems):
    cut = first_ref.shape[1]
    copies = [
        pltpu.make_async_copy(tables_ref.at[1, :, :cut], first_ref, sems.at[0]),
        pltpu.make_async_copy(tables_ref.at[1, :, cut:], second_ref, sems.at[1]),
        pltpu.make_async_copy(tables_ref.at[0], a_ref, sems.at[2]),
    ]
    for c in copies:
        c.start()
    for c in copies:
        c.wait()


def load_tables(tables, cut):
    if INTERPRET:
        return tables[0], tables[1][:, :cut], tables[1][:, cut:]
    _, heights, half = tables.shape
    vmem = pl.BlockSpec(memory_space=pltpu.VMEM)
    return pl.pallas_call(
        load_kernel,
        out_shape=[pltpu.VMEM((heights, n), tables.dtype) for n in (half, cut, half - cut)],
        in_specs=[pl.BlockSpec(memory_space=pltpu.HBM)],
        out_specs=[vmem] * 3,
        scratch_shapes=[pltpu.SemaphoreType.DMA((3,))],
        compiler_params=pltpu.CompilerParams(vmem_limit_bytes=2 * 2**20),
    )(pltpu.with_memory_space_constraint(tables, pltpu.HBM))


def couple_kernel(own_ref, other_ref, out_ref):
    half = own_ref.shape[1]
    for cols, x in ((slice(0, half), own_ref[...]),):
        hi, lo = split(x)
        out_ref[0, :, cols] = hi
        out_ref[1, :, cols] = lo
    for into, out_of in ((slice(0, half), slice(half, 2 * half)), (slice(half, 2 * half), slice(0, half))):
        hi, lo = split(other_ref[out_of, :])
        out_ref[0, into, half:] = hi
        out_ref[1, into, half:] = lo


def row_couple_kernel(own_ref, other_ref, out_ref):
    half = own_ref.shape[0]
    hi, lo = split(own_ref[...])
    out_ref[0, :half] = hi
    out_ref[1, :half] = lo
    hi, lo = split(swap_cols(other_ref[...]))
    out_ref[0, half:] = hi
    out_ref[1, half:] = lo


def pin(x):
    if INTERPRET:
        return x
    return pl.pallas_call(
        lambda x_ref, out_ref: None,
        out_shape=pltpu.VMEM(x.shape, x.dtype),
        in_specs=[pl.BlockSpec(memory_space=pltpu.VMEM)],
        out_specs=pl.BlockSpec(memory_space=pltpu.VMEM),
        input_output_aliases={0: 0},
        compiler_params=pltpu.CompilerParams(vmem_limit_bytes=2**20),
    )(pltpu.with_memory_space_constraint(x, pltpu.VMEM))


PAD = 16


def on_diagonal(size):
    return lax.broadcasted_iota(jnp.int32, (size, size), 0) == lax.broadcasted_iota(jnp.int32, (size, size), 1)


def pack(z, ref):
    rows = z.shape[0]
    top = jnp.maximum(jnp.max(jnp.abs(z), axis=(0, 1), keepdims=True), 1e-30)
    exponent = jnp.floor(jnp.log2(top)) - 14.0
    z = z * jnp.exp2(-exponent)
    mask = on_diagonal(rows)
    diagonal = jnp.sum(jnp.where(mask, z[:, :rows], 0.0), axis=0, keepdims=True)
    hi = diagonal.astype(bf16).astype(f32)
    row = lax.broadcasted_iota(jnp.int32, (PAD, rows), 0)
    ref[:rows, :rows] = jnp.where(mask, 0.0, z[:, :rows])
    ref[:rows, rows:] = z[:, rows:]
    ref[rows:, :rows] = jnp.where(row == 0, exponent, jnp.where(row == 1, hi, diagonal - hi))
    ref[rows:, rows:] = jnp.zeros((PAD, z.shape[1] - rows), f32)


def local_kernel(ka_ref, kb_ref, g_ref, packed_ref):
    khi, klo = split(jnp.concatenate([ka_ref[...], kb_ref[...]], axis=0))
    pack(mm3(khi, klo, g_ref[0], g_ref[1]), packed_ref)


def place_panels(all_ref, slot, own_ref, other_ref):
    half = own_ref.shape[0] - PAD
    block = 128

    def rows_of(i, carry):
        at = pl.multiple_of(i * block, block)
        rows = pl.ds(at, block)
        shape = (block, half)
        mask = lax.broadcasted_iota(jnp.int32, shape, 0) + at == lax.broadcasted_iota(jnp.int32, shape, 1)
        for first, ref in ((True, own_ref), (False, other_ref)):
            scale = jnp.exp2(ref[half : half + 1, :1])
            diagonal = ref[half + 1 : half + 2, :half] + ref[half + 2 : half + 3, :half]
            left = jnp.where(mask, diagonal, ref[rows, :half]) * scale
            right = ref[rows, half:] * scale
            into = pl.ds(pl.multiple_of(at + (0 if first else half), block), block)
            for cols, x in ((slice(0, half), left if first else right), (slice(half, 2 * half), right if first else left)):
                hi, lo = split(x)
                all_ref[slot, 0, into, cols] = hi
                all_ref[slot, 1, into, cols] = lo
        return carry

    lax.fori_loop(0, half // block, rows_of, 0)


def early_kernel(*refs):
    all_ref = refs[-1]
    for n, slot in enumerate((0, 1, SIDE - 1)):
        place_panels(all_ref, slot, refs[2 * n], refs[2 * n + 1])


def group_kernel(base, last, coords_ref, _, own_ref, other_ref, all_ref, prefix_ref, out_ref, run_ref):
    place = coords_ref[base]
    half = run_ref.shape[2]
    place_panels(all_ref, 2, own_ref, other_ref)
    run_ref[1] = all_ref[place, :, :half]
    prefix_ref[0, :, :half] = jnp.where(on_diagonal(half), 1.0, 0.0).astype(bf16)
    prefix_ref[0, :, half:] = jnp.zeros((half, half), bf16)
    prefix_ref[1] = jnp.zeros((half, 2 * half), bf16)
    block = 256

    def step(n, carry):
        i = n // (2 * half // block) + 1
        cols = pl.ds(pl.multiple_of(n % (2 * half // block) * block, block), block)
        now = i % 2

        @pl.when(place == i)
        def _():
            prefix_ref[:, :, cols] = run_ref[now, :, :, cols]

        slot = coords_ref[base + i]
        hi, lo = split(mm3(run_ref[now, 0], run_ref[now, 1], all_ref[slot, 0, :, cols], all_ref[slot, 1, :, cols]))
        run_ref[1 - now, 0, :, cols] = hi
        run_ref[1 - now, 1, :, cols] = lo
        return carry

    lax.fori_loop(0, (SIDE - 1) * (2 * half // block), step, 0)
    end = SIDE % 2
    if last:
        out_ref[...] = run_ref[end]
    else:
        pack(run_ref[end, 0].astype(f32) + run_ref[end, 1].astype(f32), out_ref)


def whole(own_ref, other_ref, part):
    return jnp.concatenate([own_ref[part], swap_cols(other_ref[part])], axis=0)


def launch_kernel(own_ref, other_ref, state_ref, out_ref, window_ref):
    for part in range(2):
        window_ref[part] = whole(own_ref, other_ref, part)
    shi, slo = split(state_ref[...])
    out_ref[...] = mm3(shi, slo, window_ref[0], window_ref[1])


def hop_kernel(plane, base, coords_ref, incoming_ref, held_ref, window_ref, *rest):
    state_ref, out_ref = rest[-2:]

    @pl.when(coords_ref[base] != plane)
    def _():
        state_ref[...] = held_ref[...]
        out_ref[...] = held_ref[...]

    @pl.when(coords_ref[base] == plane)
    def _():
        incoming = incoming_ref[...]
        state_ref[...] = incoming
        shi, slo = split(incoming)
        out_ref[...] = mm3(shi, slo, window_ref[0], window_ref[1])


def last_kernel(coords_ref, v0_ref, v1_ref, v2_ref, v3_ref, ra_ref, rb_ref, ca_ref, cb_ref, k_ref, g_ref, d_ref, out_ref, v_ref):
    rows = v0_ref.shape[0]
    for r, ref in enumerate((v0_ref, v1_ref, v2_ref, v3_ref)):
        v_ref[pl.ds(pl.multiple_of(coords_ref[r] * rows, rows), rows)] = ref[...]
    v = mm3(*split(v_ref[...]), whole(ra_ref, rb_ref, 0), whole(ra_ref, rb_ref, 1))
    v = mm3(*split(v), whole(ca_ref, cb_ref, 0), whole(ca_ref, cb_ref, 1))
    v = mm3(*split(v), k_ref[0], k_ref[1])
    out_ref[0] = (v * d_ref[...]).astype(bf16)
    out_ref[1] = mm3(*split(v), g_ref[0], g_ref[1]).astype(bf16)


def grouped(packed, unit, base, coords, last):
    half, modes = packed.shape[0] - PAD, packed.shape[1]
    cut = packed.shape[0] // 32 * 16
    sent = packed.astype(jnp.float16)
    before, after = around(sent, unit, 1), around(sent, unit, -1)
    far = jnp.concatenate(
        [around(before[:cut], unit, 1), around(after[cut:], unit, -1)], axis=0
    )
    near = []
    for own, value in ((packed, sent), (None, before), (None, after)):
        near += [value.astype(f32) if own is None else own, from_partner(value).astype(f32)]
    every = call(early_kernel, (jax.ShapeDtypeStruct((SIDE, 2, modes, modes), bf16),), *near)
    panel = jax.ShapeDtypeStruct((2, half, modes), bf16)
    return call(
        functools.partial(group_kernel, base, last),
        (
            jax.ShapeDtypeStruct(every.shape, bf16),
            panel,
            panel if last else jax.ShapeDtypeStruct(packed.shape, f32),
        ),
        coords, every, far.astype(f32), from_partner(far).astype(f32),
        scratch=[pltpu.VMEM((2, 2, half, modes), bf16)], aliases={1: 0},
    )[1:]


def on_device(mode_tables, attenuation, excitation):
    _, heights, half = mode_tables.shape
    modes = 2 * half
    planes = lax.axis_size("range") // PLANE
    position = lax.axis_index("range")
    core = lax.axis_index("chip")
    x, y, z = position % SIDE, position // SIDE % SIDE, position // PLANE
    coords = jnp.stack([(w - r) % SIDE for w in (x, y) for r in range(SIDE)] + [z]).astype(jnp.int32)
    z_at = 2 * SIDE

    cuts = (0, half * 2 // 3, half)
    table_a, *table_b = load_tables(mode_tables, cuts[1])
    earlier = [from_behind(t, 1) for t in table_b]
    table_b = jnp.concatenate(table_b, axis=1)
    other_a = from_partner(table_a)
    rows = heights // 2
    theirs = lax.dynamic_slice_in_dim(table_b, (1 - core) * rows, rows, 0)
    other_rows_b = from_partner(theirs)

    damping = jnp.exp(-attenuation)
    damping = jnp.where(core == 0, damping, jnp.roll(damping, half, axis=1))
    sources = excitation.shape[1] // 2
    share = excitation.shape[1] // SIDE
    start = lax.dynamic_slice_in_dim(excitation.T, x * share + core * (share // 2), share // 2, 0)
    start = jnp.where(core == 0, start, jnp.roll(start, half, axis=1))

    def overlap(a, b):
        return jnp.einsum("hi,hj->ij", a, b, preferred_element_type=f32)

    damping_a, damping_b = damping[0], damping[1, :half]
    inner = jnp.concatenate([overlap(table_a, table_b), overlap(other_a, table_b)], axis=0)
    inner = inner * damping_a[:, None] * damping_b[None, :]
    matrix = jax.ShapeDtypeStruct((2, modes, modes), bf16)
    inner = call(couple_kernel, (matrix,), inner, from_partner(inner))
    both_a = jnp.concatenate([table_a, other_a], axis=1)
    own_rows = lax.dynamic_slice_in_dim(jnp.stack([table_a, table_b]), core * rows, rows, 1)
    other_rows_a = lax.dynamic_slice_in_dim(other_a, core * rows, rows, 0)
    whole_rows = jnp.concatenate([own_rows, jnp.stack([other_rows_a, other_rows_b])], axis=2)
    earlier[0], both_a, whole_rows, start, inner, coords = lax.optimization_barrier(
        (earlier[0], both_a, whole_rows, start, inner, coords)
    )

    k = [
        jnp.where(position == 0, jnp.eye(hi - lo, modes, lo, dtype=f32), overlap(e, both_a))
        for e, lo, hi in zip(earlier, cuts, cuts[1:])
    ]
    packed = jax.ShapeDtypeStruct((half + PAD, modes), f32)
    packed = call(local_kernel, (packed,), *k, inner)
    k = jnp.concatenate(k, axis=0)
    k = call(row_couple_kernel, (matrix,), k, from_partner(k))
    in_row, packed = grouped(packed, 1, 0, coords, False)
    in_row_other = from_partner(in_row)
    packed, k, in_row_other = lax.optimization_barrier((packed, k, in_row_other))
    of_rows, window = grouped(packed, SIDE, SIDE, coords, True)
    held = start
    of_rows_other = from_partner(of_rows)
    finish = (of_rows, of_rows_other, in_row, in_row_other, k, inner)
    state = jax.ShapeDtypeStruct((share // 2, modes), f32)
    out, window = call(launch_kernel, (state, matrix), window, from_partner(window), held)
    for n in range(1, planes - 1):
        incoming = from_behind(out, PLANE)
        held, out = call(
            functools.partial(hop_kernel, n, z_at), (state, state), coords, incoming, held, window,
            *(finish if n == planes // 2 else ()),
        )
    held = jnp.where(z == planes - 1, from_behind(out, PLANE), held)
    held = pin(held)
    parts = [held] + [pin(around(held, 1, r)) for r in range(1, SIDE)]
    amplitude = call(
        last_kernel,
        (jax.ShapeDtypeStruct((2, sources, modes), bf16),),
        coords, *parts, *finish, damping[:1],
        scratch=[pltpu.VMEM((sources, modes), f32)],
    )
    others = from_partner(amplitude)
    others = jnp.concatenate([others[:, :, half:], others[:, :, :half]], axis=2)
    low, high = jnp.where(core == 0, amplitude, others), jnp.where(core == 0, others, amplitude)
    both = [v.reshape(2, SIDE, share // 2, modes) for v in (low, high)]
    amplitude = jnp.stack(both, axis=2).reshape(2, 2 * sources, modes)
    return jnp.einsum("shm,scm->shc", whole_rows, amplitude, preferred_element_type=f32)


def solution(mesh):
    placed = (P("range", None, "chip"), P("range", None), P())
    return jax.shard_map(
        on_device, mesh=mesh, in_specs=placed, out_specs=P("range", "chip", None), check_vma=False
    )
```

```python
import functools

import jax
import jax.numpy as jnp
from jax import lax
from jax.experimental import pallas as pl
from jax.experimental.pallas import tpu as pltpu
from jax.sharding import PartitionSpec as P

INTERPRET = False
f32, bf16 = jnp.float32, jnp.bfloat16


SIDE = 4
PLANE = SIDE * SIDE


def from_behind(value, steps):
    count = lax.axis_size("range")
    return lax.ppermute(value, "range", [(i, (i + steps) % count) for i in range(count)])


def around(value, unit, steps):
    count = lax.axis_size("range")

    def target(i):
        place = i // unit % SIDE
        return i + unit * ((place + steps) % SIDE - place)

    return lax.ppermute(value, "range", [(i, target(i)) for i in range(count)])


def from_partner(value):
    return lax.ppermute(value, "chip", [(0, 1), (1, 0)])


def split(x):
    hi = x.astype(bf16)
    return hi, (x - hi.astype(f32)).astype(bf16)


def mm(a, b):
    return jnp.dot(a, b, preferred_element_type=f32)


def mm3(lhi, llo, rhi, rlo):
    rows = lhi.shape[0]
    both = mm(jnp.concatenate([lhi, llo], axis=0), rhi)
    return both[:rows] + (both[rows:] + mm(lhi, rlo))


BLOCK = 256


def product(left_ref, right_ref, store):
    def step(j, carry):
        cols = pl.ds(pl.multiple_of(j * BLOCK, BLOCK), BLOCK)
        store(cols, mm3(left_ref[0], left_ref[1], right_ref[0, :, cols], right_ref[1, :, cols]))
        return carry

    lax.fori_loop(0, right_ref.shape[2] // BLOCK, step, 0)


def keep(ref, x):
    hi, lo = split(x)
    ref[0] = hi
    ref[1] = lo


def join(into_ref, own_ref, other_ref):
    half, block = own_ref.shape[1], 128

    def step(i, carry):
        rows = pl.ds(pl.multiple_of(i * block, block), block)
        below = pl.ds(pl.multiple_of(half + i * block, block), block)
        for part in range(2):
            into_ref[part, rows] = own_ref[part, rows]
            into_ref[part, below, :half] = other_ref[part, rows, half:]
            into_ref[part, below, half:] = other_ref[part, rows, :half]
        return carry

    lax.fori_loop(0, half // block, step, 0)


def swap_cols(x):
    half = x.shape[1] // 2
    return jnp.concatenate([x[:, half:], x[:, :half]], axis=1)


def call(kernel, out, *args, scratch=(), limit=12, aliases=None):
    in_specs = [
        pl.BlockSpec(memory_space=pltpu.SMEM if a.dtype == jnp.int32 else pltpu.VMEM) for a in args
    ]
    out_specs = [pl.BlockSpec(memory_space=pltpu.VMEM) for _ in out]
    shapes = list(out)
    if not INTERPRET:
        shapes = [pltpu.VMEM(o.shape, o.dtype) for o in out]
        args = [
            a if a.dtype == jnp.int32 else pltpu.with_memory_space_constraint(a, pltpu.VMEM) for a in args
        ]
    outs = pl.pallas_call(
        kernel, out_shape=shapes, in_specs=in_specs, out_specs=out_specs, interpret=INTERPRET,
        compiler_params=pltpu.CompilerParams(vmem_limit_bytes=limit * 2**20),
        scratch_shapes=scratch,
        input_output_aliases=aliases or {},
    )(*args)
    return outs if len(out) > 1 else outs[0]


def load_kernel(tables_ref, a_ref, b_ref, sems):
    copies = [
        pltpu.make_async_copy(tables_ref.at[1], b_ref, sems.at[0]),
        pltpu.make_async_copy(tables_ref.at[0], a_ref, sems.at[1]),
    ]
    for c in copies:
        c.start()
    for c in copies:
        c.wait()


def load_tables(tables):
    if INTERPRET:
        return tables[0], tables[1]
    vmem = pl.BlockSpec(memory_space=pltpu.VMEM)
    return pl.pallas_call(
        load_kernel,
        out_shape=[pltpu.VMEM(tables.shape[1:], tables.dtype)] * 2,
        in_specs=[pl.BlockSpec(memory_space=pltpu.HBM)],
        out_specs=[vmem] * 2,
        scratch_shapes=[pltpu.SemaphoreType.DMA((2,))],
        compiler_params=pltpu.CompilerParams(vmem_limit_bytes=2 * 2**20),
    )(pltpu.with_memory_space_constraint(tables, pltpu.HBM))


def couple_kernel(own_ref, other_ref, out_ref):
    half = own_ref.shape[1]
    for cols, x in ((slice(0, half), own_ref[...]),):
        hi, lo = split(x)
        out_ref[0, :, cols] = hi
        out_ref[1, :, cols] = lo
    for into, out_of in ((slice(0, half), slice(half, 2 * half)), (slice(half, 2 * half), slice(0, half))):
        hi, lo = split(other_ref[out_of, :])
        out_ref[0, into, half:] = hi
        out_ref[1, into, half:] = lo


def row_couple_kernel(own_ref, other_ref, out_ref):
    half = own_ref.shape[0]
    hi, lo = split(own_ref[...])
    out_ref[0, :half] = hi
    out_ref[1, :half] = lo
    hi, lo = split(swap_cols(other_ref[...]))
    out_ref[0, half:] = hi
    out_ref[1, half:] = lo


def pin(x):
    if INTERPRET:
        return x
    return pl.pallas_call(
        lambda x_ref, out_ref: None,
        out_shape=pltpu.VMEM(x.shape, x.dtype),
        in_specs=[pl.BlockSpec(memory_space=pltpu.VMEM)],
        out_specs=pl.BlockSpec(memory_space=pltpu.VMEM),
        input_output_aliases={0: 0},
        compiler_params=pltpu.CompilerParams(vmem_limit_bytes=2**20),
    )(pltpu.with_memory_space_constraint(x, pltpu.VMEM))


PAD = 16


def on_diagonal(size):
    return lax.broadcasted_iota(jnp.int32, (size, size), 0) == lax.broadcasted_iota(jnp.int32, (size, size), 1)


def pack(ref):
    rows = ref.shape[0] - PAD
    z = ref[:rows]
    top = jnp.maximum(jnp.max(jnp.abs(z), axis=(0, 1), keepdims=True), 1e-30)
    exponent = jnp.floor(jnp.log2(top)) - 14.0
    scale = jnp.exp2(-exponent)
    mask = on_diagonal(rows)
    diagonal = jnp.sum(jnp.where(mask, ref[:rows, :rows], 0.0), axis=0, keepdims=True) * scale
    hi = diagonal.astype(bf16).astype(f32)
    row = lax.broadcasted_iota(jnp.int32, (PAD, rows), 0)
    ref[:rows, :rows] = jnp.where(mask, 0.0, ref[:rows, :rows]) * scale
    ref[:rows, rows:] = ref[:rows, rows:] * scale
    ref[rows:, :rows] = jnp.where(row == 0, exponent, jnp.where(row == 1, hi, diagonal - hi))
    ref[rows:, rows:] = jnp.zeros((PAD, ref.shape[1] - rows), f32)


def local_kernel(k_in_ref, g_ref, packed_ref, k_ref):
    rows = k_ref.shape[1]
    keep(k_ref, k_in_ref[...])

    def store(cols, z):
        packed_ref[:rows, cols] = z

    product(k_ref, g_ref, store)
    pack(packed_ref)


def place_panels(all_ref, slot, own_ref, other_ref):
    half = own_ref.shape[0] - PAD
    block = 64

    def rows_of(i, carry):
        at = pl.multiple_of(i * block, block)
        rows = pl.ds(at, block)
        shape = (block, half)
        mask = lax.broadcasted_iota(jnp.int32, shape, 0) + at == lax.broadcasted_iota(jnp.int32, shape, 1)
        for first, ref in ((True, own_ref), (False, other_ref)):
            scale = jnp.exp2(ref[half : half + 1, :1])
            diagonal = ref[half + 1 : half + 2, :half] + ref[half + 2 : half + 3, :half]
            left = jnp.where(mask, diagonal, ref[rows, :half]) * scale
            right = ref[rows, half:] * scale
            into = pl.ds(pl.multiple_of(at + (0 if first else half), block), block)
            for cols, x in ((slice(0, half), left if first else right), (slice(half, 2 * half), right if first else left)):
                hi, lo = split(x)
                all_ref[slot, 0, into, cols] = hi
                all_ref[slot, 1, into, cols] = lo
        return carry

    lax.fori_loop(0, half // block, rows_of, 0)


def early_kernel(own_ref, other_ref, own_near_ref, other_near_ref, all_ref):
    rows = own_ref.shape[0]
    place_panels(all_ref, 0, own_ref, other_ref)
    for n, slot in enumerate((1, SIDE - 1)):
        at = slice(n * rows, (n + 1) * rows)
        place_panels(all_ref, slot, own_near_ref.at[at], other_near_ref.at[at])


def group_kernel(base, last, coords_ref, _, own_ref, other_ref, all_ref, prefix_ref, out_ref, run_ref):
    place = coords_ref[base]
    half = run_ref.shape[2]
    place_panels(all_ref, 2, own_ref, other_ref)
    run_ref[1] = all_ref[place, :, :half]
    prefix_ref[0, :, :half] = jnp.where(on_diagonal(half), 1.0, 0.0).astype(bf16)
    prefix_ref[0, :, half:] = jnp.zeros((half, half), bf16)
    prefix_ref[1] = jnp.zeros((half, 2 * half), bf16)
    block = 256

    def step(n, carry):
        i = n // (2 * half // block) + 1
        cols = pl.ds(pl.multiple_of(n % (2 * half // block) * block, block), block)
        now = i % 2

        @pl.when(place == i)
        def _():
            prefix_ref[:, :, cols] = run_ref[now, :, :, cols]

        slot = coords_ref[base + i]
        hi, lo = split(mm3(run_ref[now, 0], run_ref[now, 1], all_ref[slot, 0, :, cols], all_ref[slot, 1, :, cols]))
        run_ref[1 - now, 0, :, cols] = hi
        run_ref[1 - now, 1, :, cols] = lo
        return carry

    lax.fori_loop(0, (SIDE - 1) * (2 * half // block), step, 0)
    end = SIDE % 2
    if last:
        out_ref[...] = run_ref[end]
    else:
        out_ref[:half] = run_ref[end, 0].astype(f32) + run_ref[end, 1].astype(f32)
        pack(out_ref)


def launch_kernel(own_ref, other_ref, state_ref, out_ref, window_ref, left_ref):
    join(window_ref, own_ref, other_ref)
    keep(left_ref, state_ref[...])

    def store(cols, z):
        out_ref[:, cols] = z

    product(left_ref, window_ref, store)


def hop_kernel(plane, base, coords_ref, incoming_ref, held_ref, window_ref, state_ref, out_ref, left_ref):
    @pl.when(coords_ref[base] != plane)
    def _():
        state_ref[...] = held_ref[...]
        out_ref[...] = held_ref[...]

    @pl.when(coords_ref[base] == plane)
    def _():
        state_ref[...] = incoming_ref[...]
        keep(left_ref, incoming_ref[...])

        def store(cols, z):
            out_ref[:, cols] = z

        product(left_ref, window_ref, store)


def last_kernel(coords_ref, v0_ref, v1_ref, v2_ref, v3_ref, ra_ref, rb_ref, ca_ref, cb_ref, k_ref, g_ref, d_ref, out_ref, v_ref, left_ref, w_ref):
    rows = v0_ref.shape[0]
    for r, ref in enumerate((v0_ref, v1_ref, v2_ref, v3_ref)):
        v_ref[pl.ds(pl.multiple_of(coords_ref[r] * rows, rows), rows)] = ref[...]

    def store(cols, z):
        v_ref[:, cols] = z

    for pair in ((ra_ref, rb_ref), (ca_ref, cb_ref)):
        join(w_ref, *pair)
        keep(left_ref, v_ref[...])
        product(left_ref, w_ref, store)
    keep(left_ref, v_ref[...])
    product(left_ref, k_ref, store)
    out_ref[0] = (v_ref[...] * d_ref[...]).astype(bf16)
    keep(left_ref, v_ref[...])

    def store_second(cols, z):
        out_ref[1, :, cols] = z.astype(bf16)

    product(left_ref, g_ref, store_second)


def grouped(packed, unit, base, coords, last):
    half, modes = packed.shape[0] - PAD, packed.shape[1]
    cut = packed.shape[0] // 32 * 16
    sent = packed.astype(jnp.float16)
    before, after = around(sent, unit, 1), around(sent, unit, -1)
    far = jnp.concatenate(
        [around(before[:cut], unit, 1), around(after[cut:], unit, -1)], axis=0
    )
    near = jnp.concatenate([before, after], axis=0)
    near = [packed, from_partner(sent).astype(f32), near.astype(f32), from_partner(near).astype(f32)]
    every = call(early_kernel, (jax.ShapeDtypeStruct((SIDE, 2, modes, modes), bf16),), *near)
    panel = jax.ShapeDtypeStruct((2, half, modes), bf16)
    return call(
        functools.partial(group_kernel, base, last),
        (
            jax.ShapeDtypeStruct(every.shape, bf16),
            panel,
            panel if last else jax.ShapeDtypeStruct(packed.shape, f32),
        ),
        coords, every, far.astype(f32), from_partner(far).astype(f32),
        scratch=[pltpu.VMEM((2, 2, half, modes), bf16)], aliases={1: 0},
    )[1:]


def on_device(mode_tables, attenuation, excitation):
    _, heights, half = mode_tables.shape
    modes = 2 * half
    planes = lax.axis_size("range") // PLANE
    position = lax.axis_index("range")
    core = lax.axis_index("chip")
    x, y, z = position % SIDE, position // SIDE % SIDE, position // PLANE
    coords = jnp.stack([(w - r) % SIDE for w in (x, y) for r in range(SIDE)] + [z]).astype(jnp.int32)
    z_at = 2 * SIDE

    table_a, table_b = load_tables(mode_tables)
    earlier = from_behind(table_b, 1)
    other_a = from_partner(table_a)
    rows = heights // 2
    theirs = lax.dynamic_slice_in_dim(table_b, (1 - core) * rows, rows, 0)
    other_rows_b = from_partner(theirs)

    damping = jnp.exp(-attenuation)
    damping = jnp.where(core == 0, damping, jnp.roll(damping, half, axis=1))
    sources = excitation.shape[1] // 2
    share = excitation.shape[1] // SIDE
    start = lax.dynamic_slice_in_dim(excitation.T, x * share + core * (share // 2), share // 2, 0)
    start = jnp.where(core == 0, start, jnp.roll(start, half, axis=1))

    def overlap(a, b):
        return jnp.einsum("hi,hj->ij", a, b, preferred_element_type=f32)

    damping_a, damping_b = damping[0], damping[1, :half]
    inner = jnp.concatenate([overlap(table_a, table_b), overlap(other_a, table_b)], axis=0)
    inner = inner * damping_a[:, None] * damping_b[None, :]
    matrix = jax.ShapeDtypeStruct((2, modes, modes), bf16)
    inner = call(couple_kernel, (matrix,), inner, from_partner(inner))
    both_a = jnp.concatenate([table_a, other_a], axis=1)
    own_rows = lax.dynamic_slice_in_dim(jnp.stack([table_a, table_b]), core * rows, rows, 1)
    other_rows_a = lax.dynamic_slice_in_dim(other_a, core * rows, rows, 0)
    whole_rows = jnp.concatenate([own_rows, jnp.stack([other_rows_a, other_rows_b])], axis=2)
    earlier, both_a, whole_rows, start, inner, coords = lax.optimization_barrier(
        (earlier, both_a, whole_rows, start, inner, coords)
    )

    k = jnp.where(position == 0, jnp.eye(half, modes, dtype=f32), overlap(earlier, both_a))
    packed = jax.ShapeDtypeStruct((half + PAD, modes), f32)
    packed = call(local_kernel, (packed,), k, inner, scratch=[pltpu.VMEM((2, half, modes), bf16)])
    k = call(row_couple_kernel, (matrix,), k, from_partner(k))
    in_row, packed = grouped(packed, 1, 0, coords, False)
    in_row_other = from_partner(in_row)
    packed, k, in_row_other = lax.optimization_barrier((packed, k, in_row_other))
    of_rows, window = grouped(packed, SIDE, SIDE, coords, True)
    held = start
    of_rows_other = from_partner(of_rows)
    finish = (of_rows, of_rows_other, in_row, in_row_other, k, inner)
    state = jax.ShapeDtypeStruct((share // 2, modes), f32)
    out, window = call(launch_kernel, (state, matrix), window, from_partner(window), held, scratch=[pltpu.VMEM((2, share // 2, modes), bf16)])
    for n in range(1, planes - 1):
        incoming = from_behind(out, PLANE)
        held, out = call(
            functools.partial(hop_kernel, n, z_at), (state, state), coords, incoming, held, window,
            scratch=[pltpu.VMEM((2, share // 2, modes), bf16)],
        )
    held = jnp.where(z == planes - 1, from_behind(out, PLANE), held)
    held = pin(held)
    parts = [held] + [pin(around(held, 1, r)) for r in range(1, SIDE)]
    amplitude = call(
        last_kernel,
        (jax.ShapeDtypeStruct((2, sources, modes), bf16),),
        coords, *parts, *finish, damping[:1],
        scratch=[
            pltpu.VMEM((sources, modes), f32),
            pltpu.VMEM((2, sources, modes), bf16),
            pltpu.VMEM((2, modes, modes), bf16),
        ],
    )
    others = from_partner(amplitude)
    others = jnp.concatenate([others[:, :, half:], others[:, :, :half]], axis=2)
    low, high = jnp.where(core == 0, amplitude, others), jnp.where(core == 0, others, amplitude)
    both = [v.reshape(2, SIDE, share // 2, modes) for v in (low, high)]
    amplitude = jnp.stack(both, axis=2).reshape(2, 2 * sources, modes)
    return jnp.einsum("shm,scm->shc", whole_rows, amplitude, preferred_element_type=f32)


def solution(mesh):
    placed = (P("range", None, "chip"), P("range", None), P())
    return jax.shard_map(
        on_device, mesh=mesh, in_specs=placed, out_specs=P("range", "chip", None), check_vma=False
    )
```
